32 devices in a mesh: part: 1 (over z), tp: 4 (over y), dp: 8 (over x, core).
Axes of the slice: x: 4, y: 4, z: 1, core: 2. Of those that a mesh axis runs over, the one named last changes fastest.
The devices are a block of a 4x4x8 slice.
Arguments:
- hidden: bfloat16 [32, 2048, 2048], P(('part', 'dp', 'tp'))
- ln_gain: float32 [2048], replicated
- w_in: bfloat16 [2048, 18944], P(None, ('dp', 'tp'))
- w_out: bfloat16 [10240, 2048], P(('dp', 'tp'))
Outputs:
- output 1: bfloat16 [32, 2048, 2048], P(('part', 'dp', 'tp'))
- output 2: bfloat16 [32, 2048, 256], P(('part', 'dp', 'tp'))
- output 3: bfloat16 [32, 2048, 256], P(('part', 'dp', 'tp'))
All inputs are finite; a program needn't handle non-finite values.
Results may differ from the reference program's by a relative error of at most 0.00278234.
Values are sent between devices in bfloat16 or wider.
A program may use at most 768 MiB of HBM per device.

```python
import jax
import jax.numpy as jnp
from jax import lax

D = 2048
HEADS = 8
HEAD = 256
BATCH = 32
SEQ = 2048

FF = 4 * D
Q_WIDTH = HEADS * HEAD
JOINT = Q_WIDTH + 2 * HEAD + 2 * FF
MIXED = Q_WIDTH + FF
Q_BLOCK = min(SEQ, 512)
LN_EPS = 1e-6
ROPE_BASE = 10000.0
ATTN_GAIN = 3.0


def setup_inputs(seed: int = 0, part: int = 0) -> dict:
    root_key = jax.random.key(seed)
    key_hidden, key_gain, key_in, key_out = jax.random.split(root_key, 4)
    key_hidden = jax.random.fold_in(key_hidden, part)
    hidden = jax.random.normal(key_hidden, (BATCH, SEQ, D), jnp.float32)
    ln_gain = 1.0 + 0.25 * jax.random.normal(key_gain, (D,), jnp.float32)
    w_in = jax.random.normal(key_in, (D, JOINT), jnp.float32) * D ** -0.5
    row_scale = jnp.where(jnp.arange(MIXED) < Q_WIDTH, ATTN_GAIN, 1.0) * MIXED ** -0.5
    w_out = jax.random.normal(key_out, (MIXED, D), jnp.float32) * row_scale[:, None]
    return {'hidden': hidden.astype(jnp.bfloat16), 'ln_gain': ln_gain,
            'w_in': w_in.astype(jnp.bfloat16), 'w_out': w_out.astype(jnp.bfloat16)}


def rotate(values):
    half_dim = HEAD // 2
    inv_freq = ROPE_BASE ** (-jnp.arange(half_dim, dtype=jnp.float32) * 2.0 / HEAD)
    angles = jnp.arange(SEQ, dtype=jnp.float32)[:, None] * inv_freq[None, :]
    tab_shape = (SEQ,) + (1,) * (values.ndim - 2) + (half_dim,)
    cos_tab = jnp.cos(angles).reshape(tab_shape)
    sin_tab = jnp.sin(angles).reshape(tab_shape)
    first_half = values[..., :half_dim]
    second_half = values[..., half_dim:]
    return jnp.concatenate([first_half * cos_tab - second_half * sin_tab,
                            second_half * cos_tab + first_half * sin_tab], axis=-1)


def attention(q_rot, k_rot, v_seq):
    k_wide = k_rot.astype(jnp.float32)
    v_wide = v_seq.astype(jnp.float32)
    key_pos = jnp.arange(SEQ)
    q_blocks = q_rot.reshape(SEQ // Q_BLOCK, Q_BLOCK, HEADS, HEAD)

    def one_block(item):
        blk_idx, q_tile = item
        scores = jnp.einsum('qhe,ke->qhk', q_tile.astype(jnp.float32), k_wide) * HEAD ** -0.5
        q_pos = blk_idx * Q_BLOCK + jnp.arange(Q_BLOCK)
        allowed = key_pos[None, :] <= q_pos[:, None]
        scores = jnp.where(allowed[:, None, :], scores, -1e30)
        attn_prob = jax.nn.softmax(scores, axis=-1).astype(jnp.bfloat16)
        return jnp.einsum('qhk,ke->qhe', attn_prob.astype(jnp.float32), v_wide).astype(jnp.bfloat16)

    out_tiles = lax.map(one_block, (jnp.arange(SEQ // Q_BLOCK), q_blocks))
    return out_tiles.reshape(SEQ, Q_WIDTH)


def reference(hidden, ln_gain, w_in, w_out):
    def one_request(x_seq):
        x_wide = x_seq.astype(jnp.float32)
        centered = x_wide - jnp.mean(x_wide, axis=-1, keepdims=True)
        row_var = jnp.mean(centered * centered, axis=-1, keepdims=True)
        h_seq = (centered * lax.rsqrt(row_var + LN_EPS) * ln_gain).astype(jnp.bfloat16)
        joint_out = jnp.dot(h_seq, w_in, preferred_element_type=jnp.float32).astype(jnp.bfloat16)
        q_raw = joint_out[:, :Q_WIDTH].reshape(SEQ, HEADS, HEAD)
        k_raw = joint_out[:, Q_WIDTH:Q_WIDTH + HEAD]
        v_seq = joint_out[:, Q_WIDTH + HEAD:Q_WIDTH + 2 * HEAD]
        gate_proj = joint_out[:, Q_WIDTH + 2 * HEAD:Q_WIDTH + 2 * HEAD + FF]
        up_proj = joint_out[:, Q_WIDTH + 2 * HEAD + FF:]
        q_rot = rotate(q_raw.astype(jnp.float32)).astype(jnp.bfloat16)
        k_rot = rotate(k_raw.astype(jnp.float32)).astype(jnp.bfloat16)
        attn_out = attention(q_rot, k_rot, v_seq)
        mlp_out = (jax.nn.silu(gate_proj.astype(jnp.float32)) * up_proj.astype(jnp.float32)).astype(jnp.bfloat16)
        mixed_rows = jnp.concatenate([attn_out, mlp_out], axis=-1)
        proj_out = jnp.dot(mixed_rows, w_out, preferred_element_type=jnp.float32)
        y_seq = (x_wide + proj_out).astype(jnp.bfloat16)
        return (y_seq, k_rot, v_seq)

    y_all, k_all, v_all = lax.map(one_request, hidden)
    return (y_all, k_all, v_all)
```

```python
import functools

import jax
import jax.numpy as jnp
from jax import lax
from jax.experimental import pallas as pl
from jax.experimental.pallas import tpu as pltpu
from jax.sharding import PartitionSpec as P

LN_EPS = 1e-6
ROPE_BASE = 10000.0


def layer_norm(x, ln_gain):
    x_wide = x.astype(jnp.float32)
    centered = x_wide - jnp.mean(x_wide, axis=-1, keepdims=True)
    row_var = jnp.mean(centered * centered, axis=-1, keepdims=True)
    return (centered * lax.rsqrt(row_var + LN_EPS) * ln_gain).astype(jnp.bfloat16)


def rope_tables(seq_len, head_dim):
    half = head_dim // 2
    inv_freq = ROPE_BASE ** (-jnp.arange(half, dtype=jnp.float32) * 2.0 / head_dim)
    angles = jnp.arange(seq_len, dtype=jnp.float32)[:, None] * inv_freq[None, :]
    return jnp.cos(angles), jnp.sin(angles)


def attention_call(rows, k_arr, v_arr, cos_tab, sin_tab, n_heads, head_dim, fresh_k):
    seq_len = rows.shape[0]
    half = head_dim // 2
    tq, kstep, pair = 256, 512, 2
    n_q, n_len = seq_len // tq, seq_len // kstep
    scale = (head_dim ** -0.5) * 1.4426950408889634

    def rope(a, cos, sin):
        a = a.astype(jnp.float32)
        lo, hi = a[:, :half], a[:, half:]
        return jnp.concatenate([lo * cos - hi * sin, hi * cos + lo * sin], axis=1).astype(jnp.bfloat16)

    def body(q_ref, k_ref, v_ref, cos_ref, sin_ref, o_ref, *caches):
        qi, hp = pl.program_id(0), pl.program_id(1)
        ks_ref, vs_ref = caches if fresh_k else (k_ref, v_ref)

        if fresh_k:
            @pl.when(jnp.logical_and(qi == 0, hp == 0))
            def _():
                def one(j, c):
                    r = pl.ds(pl.multiple_of(j * kstep, kstep), kstep)
                    ks_ref[r, :] = rope(k_ref[r, :], cos_ref[r, :], sin_ref[r, :])
                    vs_ref[r, :] = v_ref[r, :]
                    return c
                lax.fori_loop(0, n_len, one, 0)

        trow = pl.ds(pl.multiple_of(qi * tq, tq), tq)
        cos, sin = cos_ref[trow, :], sin_ref[trow, :]

        def span(length):
            keys = ks_ref[0:length, :]
            vals = vs_ref[0:length, :]
            k_pos = (length - kstep) + lax.broadcasted_iota(jnp.int32, (tq, kstep), 1)
            q_pos = qi * tq + lax.broadcasted_iota(jnp.int32, (tq, kstep), 0)
            allowed = k_pos <= q_pos
            for j in range(pair):
                cols = slice(j * head_dim, (j + 1) * head_dim)
                q = rope(q_ref[:, cols], cos, sin)
                s = lax.dot_general(q, keys, (((1,), (1,)), ((), ())), preferred_element_type=jnp.float32) * scale
                last = jnp.where(allowed, s[:, length - kstep:], -1e30)
                s = jnp.concatenate([s[:, :length - kstep], last], axis=1) if length > kstep else last
                top = jnp.max(s, axis=1, keepdims=True)
                e = jnp.exp2(s - top)
                tot = jnp.sum(e, axis=1, keepdims=True)
                pr = (e * (1.0 / tot)).astype(jnp.bfloat16)
                o_ref[:, cols] = jnp.dot(pr, vals, preferred_element_type=jnp.float32).astype(jnp.bfloat16)

        for b in range(n_len):
            pl.when(qi // (kstep // tq) == b)(functools.partial(span, (b + 1) * kstep))

    whole = pl.BlockSpec((seq_len, head_dim), lambda i, h: (0, 0))
    tab = pl.BlockSpec((seq_len, half), lambda i, h: (0, 0))
    out_specs = [pl.BlockSpec((tq, pair * head_dim), lambda i, h: (i, h))]
    out_shape = [jax.ShapeDtypeStruct((seq_len, n_heads * head_dim), jnp.bfloat16)]
    if fresh_k:
        k_arr = v_arr = rows
        kv_specs = [pl.BlockSpec((seq_len, head_dim), lambda i, h: (0, n_heads)),
                    pl.BlockSpec((seq_len, head_dim), lambda i, h: (0, n_heads + 1))]
        out_specs += [whole, whole]
        out_shape += [jax.ShapeDtypeStruct((seq_len, head_dim), jnp.bfloat16)] * 2
    else:
        kv_specs = [whole, whole]
    flops = 4 * n_heads * seq_len * seq_len * head_dim * 5 // 8
    return pl.pallas_call(
        body,
        grid=(n_q, n_heads // pair),
        in_specs=[pl.BlockSpec((tq, pair * head_dim), lambda i, h: (i, h))] + kv_specs + [tab, tab],
        out_specs=out_specs,
        out_shape=out_shape,
        compiler_params=pltpu.CompilerParams(dimension_semantics=("arbitrary", "arbitrary"),
                                             vmem_limit_bytes=40 * 1024 * 1024),
        cost_estimate=pl.CostEstimate(flops=flops, bytes_accessed=16 * 1024 * 1024, transcendentals=0),
        name="mqa_a" if fresh_k else "mqa_b",
    )(rows, k_arr, v_arr, cos_tab, sin_tab)


def in_proj_call(chunk, h_t, p_t, dep, first, n_dev, block, offset, name):
    rows = chunk.shape[0] // n_dev
    depth, n_tok = h_t.shape
    n_grp = n_dev - first
    g = next(c for c in (7, 4, 2, 1) if n_grp % c == 0)
    steps = n_grp // g
    m = g * rows
    tn = min(512, n_tok)
    n_in = 2 + (p_t is not None) + (dep is not None)

    def body(*refs):
        chunk_ref, h_ref = refs[0], refs[1]
        out_ref, lbuf, obuf, lsem, osem = refs[n_in:]

        def load(s):
            return pltpu.make_async_copy(chunk_ref.at[pl.ds(first * rows + s * m, m), :], lbuf.at[s % 2], lsem.at[s % 2])

        def stores(s):
            return [pltpu.make_async_copy(obuf.at[s % 2, pl.ds(i * rows, rows), :],
                                          out_ref.at[pl.ds((s * g + i) * block + offset, rows), :],
                                          osem.at[s % 2, i]) for i in range(g)]

        load(0).start()
        for s in range(steps):
            if s + 1 < steps:
                load(s + 1).start()
            load(s).wait()
            if s >= 2:
                for c in stores(s - 2):
                    c.wait()

            def tile(n, carry):
                cols = pl.ds(pl.multiple_of(n * tn, tn), tn)
                obuf[s % 2, :, cols] = jnp.dot(lbuf[s % 2], h_ref[:, cols],
                                               preferred_element_type=jnp.float32).astype(jnp.bfloat16)
                return carry
            lax.fori_loop(0, n_tok // tn, tile, 0)
            for c in stores(s):
                c.start()
        for s in range(max(0, steps - 2), steps):
            for c in stores(s):
                c.wait()

    any_spec = pl.BlockSpec(memory_space=pl.ANY)
    args, specs, alias = [chunk, h_t], [any_spec, pl.BlockSpec(memory_space=pltpu.VMEM)], {}
    if p_t is not None:
        alias = {len(args): 0}
        args.append(p_t)
        specs.append(any_spec)
    if dep is not None:
        args.append(dep)
        specs.append(any_spec)
    total = n_grp * block
    return pl.pallas_call(
        body,
        in_specs=specs,
        out_specs=any_spec,
        out_shape=jax.ShapeDtypeStruct((total, n_tok), jnp.bfloat16),
        input_output_aliases=alias,
        scratch_shapes=[pltpu.VMEM((2, m, depth), jnp.bfloat16), pltpu.VMEM((2, m, n_tok), jnp.bfloat16),
                        pltpu.SemaphoreType.DMA((2,)), pltpu.SemaphoreType.DMA((2, g))],
        compiler_params=pltpu.CompilerParams(vmem_limit_bytes=48 * 1024 * 1024),
        cost_estimate=pl.CostEstimate(flops=2 * n_grp * rows * depth * n_tok,
                                      bytes_accessed=2 * n_grp * rows * (depth + n_tok), transcendentals=0),
        name=name,
    )(*args)


PIECE = 64


def out_proj_call(p_t, w_chunk, at, per, per_dev, q_width, gate_at, ff, acc, last):
    n_tok, d_out = p_t.shape[1], w_chunk.shape[1]
    n_all = w_chunk.shape[0] // PIECE
    q_pieces = q_width // PIECE
    full, tail = 8, 4
    first = sum(1 for z in range(q_pieces) if at <= z % per_dev < at + per)
    count = n_all - first
    steps, rest = divmod(count, full)
    assert rest in (0, tail)
    kk = full * PIECE
    tt = min(512, n_tok)
    n_t = n_tok // tt

    def body(*refs):
        if last is None:
            p_ref, w_ref, out_ref, acc_ref, gbuf, ubuf, wbuf, sem = refs
        else:
            (p_ref, w_ref, accin_ref, w0_ref, a0_ref, a1_ref, x_ref, out_ref,
             acc_ref, gbuf, ubuf, wbuf, sem, abuf, xbuf, asem, xsem, osem) = refs

        def copies(s, slot, n):
            row = pl.multiple_of((first + s * full) * PIECE, PIECE) if not isinstance(s, int) else (first + s * full) * PIECE
            res = [pltpu.make_async_copy(w_ref.at[pl.ds(row, n * PIECE), :],
                                         wbuf.at[slot, pl.ds(0, n * PIECE), :], sem.at[slot, 0])]
            for j in range(n):
                o = first + s * full + j
                dst = pl.ds(j * PIECE, PIECE)
                if isinstance(s, int):
                    row = gate_at + (per_dev * (o // per) + at + o % per - q_pieces) * PIECE
                else:
                    z = per_dev * lax.div(o, per) + at + lax.rem(o, per) - q_pieces
                    row = pl.multiple_of(gate_at + z * PIECE, PIECE)
                res.append(pltpu.make_async_copy(p_ref.at[pl.ds(row, PIECE), :], gbuf.at[slot, dst, :],
                                                 sem.at[slot, 1 + j]))
                res.append(pltpu.make_async_copy(p_ref.at[pl.ds(row + ff, PIECE), :], ubuf.at[slot, dst, :],
                                                 sem.at[slot, 1 + full + j]))
            return res

        def start(s, slot, n):
            for c in copies(s, slot, n):
                c.start()

        def finish(s, slot, n):
            for c in copies(s, slot, n):
                c.wait()

        def mlp(slot, n, fresh):
            k = n * PIECE
            for t in range(n_t):
                tok = slice(t * tt, (t + 1) * tt)
                g = gbuf[slot, 0:k, tok].astype(jnp.float32)
                u = ubuf[slot, 0:k, tok].astype(jnp.float32)
                m = (g * (1.0 / (1.0 + jnp.exp(-g))) * u).astype(jnp.bfloat16)
                prod = lax.dot_general(m, wbuf[slot, 0:k, :], (((0,), (0,)), ((), ())), preferred_element_type=jnp.float32)
                if fresh:
                    acc_ref[tok, :] = prod
                else:
                    acc_ref[tok, :] += prod

        start(0, 0, full)
        if last is not None:
            acc_in = pltpu.make_async_copy(accin_ref, acc_ref, xsem.at[0])
            acc_in.start()
            x_in = pltpu.make_async_copy(x_ref, xbuf, xsem.at[1])
            x_in.start()
            acc_in.wait()
        else:
            start(1, 1, full)
            finish(0, 0, full)
            mlp(0, full, True)
        lo = 0 if last is not None else 1

        def step(s, carry):
            slot = lax.rem(s, 2)

            @pl.when(s + 1 < steps)
            def _():
                start(s + 1, 1 - slot, full)
            if rest:
                @pl.when(s + 1 == steps)
                def _():
                    start(steps, 1 - slot, tail)
            finish(s, slot, full)
            mlp(slot, full, False)
            return carry

        lax.fori_loop(lo, steps, step, 0)
        if last is not None:
            heads = a0_ref.shape[1] // kk
            srcs = [(a0_ref, i, 0) for i in range(heads)] + [(a1_ref, i, 1) for i in range(heads)]

            def attn_copies(i):
                ref, blk, odd = srcs[i]
                slot = i % 2
                res = [pltpu.make_async_copy(ref.at[:, pl.ds(blk * kk, kk)], abuf.at[slot], asem.at[slot, 0])]
                for j in range(full):
                    half, r = divmod(j, full // 2)
                    head = 2 * (2 * blk + half) + odd
                    z = head * (full // 2) + r
                    dev, loc = divmod(z, per_dev)
                    if loc < at:
                        src = w0_ref.at[pl.ds((dev * at + loc) * PIECE, PIECE), :]
                    else:
                        src = w_ref.at[pl.ds((dev * per + loc - at) * PIECE, PIECE), :]
                    res.append(pltpu.make_async_copy(src, wbuf.at[slot, pl.ds(j * PIECE, PIECE), :], asem.at[slot, 1 + j]))
                return res

        if rest:
            finish(steps, steps % 2, tail)
            mlp(steps % 2, tail, False)

        if last is None:
            out = pltpu.make_async_copy(acc_ref, out_ref, sem.at[0, 0])
            out.start()
            out.wait()
        else:
            for c in attn_copies(0):
                c.start()
            for i in range(len(srcs)):
                if i + 1 < len(srcs):
                    for c in attn_copies(i + 1):
                        c.start()
                for c in attn_copies(i):
                    c.wait()
                for t in range(n_t):
                    tok = slice(t * tt, (t + 1) * tt)
                    acc_ref[tok, :] += jnp.dot(abuf[i % 2, tok, :], wbuf[i % 2], preferred_element_type=jnp.float32)
            x_in.wait()
            outs = []
            for t in range(n_t):
                tok = slice(t * tt, (t + 1) * tt)
                xbuf[tok, :] = (xbuf[tok, :].astype(jnp.float32) + acc_ref[tok, :]).astype(jnp.bfloat16)
                c = pltpu.make_async_copy(xbuf.at[pl.ds(t * tt, tt), :], out_ref.at[pl.ds(t * tt, tt), :], osem.at[t])
                c.start()
                outs.append(c)
            for c in outs:
                c.wait()

    any_spec = pl.BlockSpec(memory_space=pl.ANY)
    args = [p_t, w_chunk]
    scratch = [pltpu.VMEM((n_tok, d_out), jnp.float32)] + [pltpu.VMEM((2, kk, n_tok), jnp.bfloat16)] * 2
    scratch += [pltpu.VMEM((2, kk, d_out), jnp.bfloat16), pltpu.SemaphoreType.DMA((2, 1 + 2 * full))]
    out_dtype = jnp.float32
    if last is not None:
        w_first, a0, a1, x = last
        args += [acc, w_first, a0, a1, x]
        scratch += [pltpu.VMEM((2, n_tok, kk), jnp.bfloat16), pltpu.VMEM((n_tok, d_out), jnp.bfloat16),
                    pltpu.SemaphoreType.DMA((2, 1 + full)), pltpu.SemaphoreType.DMA((2,)), pltpu.SemaphoreType.DMA((n_t,))]
        out_dtype = jnp.bfloat16
    k_total = count * PIECE + (q_width if last is not None else 0)
    return pl.pallas_call(
        body,
        in_specs=[any_spec] * len(args),
        out_specs=any_spec,
        out_shape=jax.ShapeDtypeStruct((n_tok, d_out), out_dtype),
        scratch_shapes=scratch,
        compiler_params=pltpu.CompilerParams(vmem_limit_bytes=60 * 1024 * 1024),
        cost_estimate=pl.CostEstimate(flops=2 * k_total * n_tok * d_out, bytes_accessed=6 * k_total * d_out, transcendentals=0),
        name="out_proj_b" if last is not None else "out_proj_a",
    )(*args)


UNIT = 16
EARLY_UNITS = (5, 8, 8)
LATE_UNITS = (11, 5)
FIRST_PIECES = 3


def solution(mesh):
    tok_spec = P(('part', 'dp', 'tp'))
    group = ('dp', 'tp')
    n_dev = mesh.shape['dp'] * mesh.shape['tp']

    def per_device(x_blk, ln_gain, w_in_blk, w_out_blk):
        x = x_blk[0]
        seq_len, d_model = x.shape
        ff = 4 * d_model
        block = w_in_blk.shape[1]
        out_block = w_out_blk.shape[0]
        q_width = out_block * n_dev - ff
        head_dim = (block * n_dev - q_width - 2 * ff) // 2
        n_heads = q_width // head_dim
        n_qkv = q_width + 2 * head_dim
        first = n_qkv // block
        gate_at = n_qkv - first * block
        early_rows = block - head_dim
        cuts = [(2 * d + 1) * head_dim - d * block for d in range(first)]
        assert 2 * first == n_heads and all(0 <= c <= early_rows for c in cuts)
        assert sum(EARLY_UNITS) * UNIT == early_rows and sum(LATE_UNITS) * UNIT == head_dim
        w_rows = w_in_blk.T
        me = lax.axis_index('dp') * mesh.shape['tp'] + lax.axis_index('tp')
        cut = jnp.where(me < first, head_dim - (block - 2 * head_dim) * me, early_rows)
        below = lax.broadcasted_iota(jnp.int32, (early_rows, 1), 0) < cut
        early_local = jnp.where(below, w_rows[:early_rows], w_rows[head_dim:])
        late_local = lax.dynamic_slice_in_dim(w_rows, cut, head_dim, axis=0)

        chunks, offset = [], 0
        for local, units in ((early_local, EARLY_UNITS), (late_local, LATE_UNITS)):
            at = 0
            for u in units:
                chunks.append((lax.all_gather(local[at:at + u * UNIT], group, axis=0, tiled=True), offset))
                at += u * UNIT
                offset += u * UNIT
        cut_out = FIRST_PIECES * PIECE
        w_out_a = lax.all_gather(w_out_blk[:cut_out], group, axis=0, tiled=True)
        w_out_b = lax.all_gather(w_out_blk[cut_out:], group, axis=0, tiled=True)

        h = layer_norm(x, ln_gain)
        h_t = h.T
        cos_tab, sin_tab = rope_tables(seq_len, head_dim)

        def head_rows(parts):
            return jnp.concatenate([c.reshape(n_dev, -1, d_model) for c, _ in parts], axis=1)

        def project(w):
            return lax.dot_general(h, w, (((1,), (1,)), ((), ())), preferred_element_type=jnp.float32).astype(jnp.bfloat16)

        n_early = len(EARLY_UNITS)
        p_t = None
        for i, (c, off) in enumerate(chunks[:n_early]):
            p_t = in_proj_call(c, h_t, p_t, None, first, n_dev, block, off, f"in_proj_{i}")
        tops = [c.reshape(n_dev, -1, d_model)[:first] for c, _ in chunks[:n_early]]
        rest, left = [], gate_at
        for c, _ in chunks[:n_early]:
            per = c.shape[0] // n_dev
            take = min(left, per)
            if take:
                rest.append(c[first * per:first * per + take])
            left -= take
        w_a = jnp.concatenate([jnp.concatenate(tops, axis=1).reshape(-1, d_model)] + rest, axis=0)
        attn_a, k_rot, v_all = attention_call(project(w_a), None, None, cos_tab, sin_tab, n_heads // 2, head_dim, True)
        dep = attn_a
        for i, (c, off) in enumerate(chunks[n_early:]):
            p_t = in_proj_call(c, h_t, p_t, dep, first, n_dev, block, off, f"in_proj_{n_early + i}")
            dep = None
        tops = [c.reshape(n_dev, -1, d_model)[:first] for c, _ in chunks[n_early:]]
        w_b = jnp.concatenate(tops, axis=1).reshape(-1, d_model)
        attn_b = attention_call(project(w_b), k_rot, v_all, cos_tab, sin_tab, n_heads // 2, head_dim, False)[0]

        per_dev = out_block // PIECE
        acc = out_proj_call(p_t, w_out_a, 0, FIRST_PIECES, per_dev, q_width, gate_at, ff, None, None)
        y = out_proj_call(p_t, w_out_b, FIRST_PIECES, per_dev - FIRST_PIECES, per_dev, q_width, gate_at, ff, acc,
                          (w_out_a, attn_a, attn_b, x))
        return y[None], k_rot[None], v_all[None]

    return jax.shard_map(per_device, mesh=mesh,
                         in_specs=(tok_spec, P(), P(None, group), P(group, None)),
                         out_specs=(tok_spec, tok_spec, tok_spec), check_vma=False)
```

```python
import functools

import jax
import jax.numpy as jnp
from jax import lax
from jax.experimental import pallas as pl
from jax.experimental.pallas import tpu as pltpu
from jax.sharding import PartitionSpec as P


MESH = pl.DeviceIdType.MESH

LN_EPS = 1e-6
ROPE_BASE = 10000.0


def rope_tables(seq_len, head_dim):
    half = head_dim // 2
    inv_freq = ROPE_BASE ** (-jnp.arange(half, dtype=jnp.float32) * 2.0 / head_dim)
    angles = jnp.arange(seq_len, dtype=jnp.float32)[:, None] * inv_freq[None, :]
    return jnp.cos(angles), jnp.sin(angles)


UNIT = 16


class Ring:
    def __init__(self, mesh_shape, shard_ref, out_ref, stage, lsem, sends, recvs, sib_sends, sib_recvs):
        self.n = mesh_shape['tp']
        self.size = mesh_shape['dp'] // 2 * self.n
        assert mesh_shape['dp'] // 2 == self.n and self.size % 2 == 0
        self.far = self.size // 2
        self.shard, self.out, self.stage, self.lsem = shard_ref, out_ref, stage, lsem
        self.sends, self.recvs, self.sib_sends, self.sib_recvs = sends, recvs, sib_sends, sib_recvs
        self.rows = shard_ref.shape[0]
        top = (self.rows // UNIT + 1) // 2 * UNIT
        self.parts = ((0, top), (top, self.rows - top))
        self.dp, self.tp = lax.axis_index('dp'), lax.axis_index('tp')
        self.core = lax.rem(self.dp, 2)
        x = lax.div(self.dp, 2)
        a = x * (1 - self.core) + self.tp * self.core
        other = self.tp * (1 - self.core) + x * self.core
        self.pos = a * self.n + lax.rem(other + a, self.n)
        self.sibling = {'dp': self.dp + 1 - 2 * self.core, 'tp': self.tp}

    def at(self, pos):
        pos = lax.rem(pos + 2 * self.size, self.size)
        a = lax.div(pos, self.n)
        other = lax.rem(lax.rem(pos, self.n) + (self.n - 1) * a, self.n)
        x = a * (1 - self.core) + other * self.core
        y = other * (1 - self.core) + a * self.core
        return 2 * x + self.core, y

    def device(self, pos):
        dp, tp = self.at(pos)
        return {'dp': dp, 'tp': tp}

    def slot(self, pos, sub):
        dp, tp = self.at(pos)
        lo, n = self.parts[sub]
        return self.out.at[pl.ds(pl.multiple_of((dp * self.n + tp) * self.rows + lo, UNIT), n), :]

    def owner(self, way, t):
        return self.pos - t if way == 0 else self.pos + t

    def hop(self, way, t, sub):
        lo, n = self.parts[sub]
        dst = self.slot(self.owner(way, t - 1), sub)
        src = dst
        if isinstance(t, int) and t == 1:
            src = self.shard.at[pl.ds(lo, n), :]
        return pltpu.make_async_remote_copy(
            src_ref=src, dst_ref=dst, send_sem=self.sends.at[way, t, sub], recv_sem=self.recvs.at[way, t, sub],
            device_id=self.device(self.pos + 1 if way == 0 else self.pos - 1), device_id_type=MESH)

    def across(self, way, t, sub):
        lo, n = self.parts[sub]
        dst = self.slot(self.owner(way, t), sub)
        src = self.shard.at[pl.ds(lo, n), :] if isinstance(t, int) and t == 0 else dst
        return pltpu.make_async_remote_copy(
            src_ref=src, dst_ref=dst, send_sem=self.sib_sends.at[way, t, sub], recv_sem=self.sib_recvs.at[way, t, sub],
            device_id=self.sibling, device_id_type=MESH)

    def begin(self):
        barrier = pltpu.get_barrier_semaphore()
        for dev in (self.device(self.pos + 1), self.device(self.pos - 1), self.sibling):
            pl.semaphore_signal(barrier, inc=1, device_id=dev, device_id_type=MESH)
        pl.semaphore_wait(barrier, 3)
        for sub in range(2):
            for way in range(2):
                self.hop(way, 1, sub).start()
        for sub in range(2):
            self.across(0, 0, sub).start()
        pltpu.make_async_copy(self.shard, self.stage, self.lsem.at[0]).start()

    def keep_own(self):
        pltpu.make_async_copy(self.shard, self.stage, self.lsem.at[0]).wait()
        dp, tp = self.at(self.pos)
        mine = self.out.at[pl.ds(pl.multiple_of((dp * self.n + tp) * self.rows, UNIT), self.rows), :]
        return pltpu.make_async_copy(self.stage, mine, self.lsem.at[1])

    def event(self, t, sub):
        def guard(cond, fn):
            if isinstance(cond, bool):
                if cond:
                    fn()
            else:
                pl.when(cond)(fn)

        for way in (0, 1):
            far = self.far if way == sub else self.far - 1

            def take(way=way, far=far):
                self.hop(way, t, sub).wait_recv()
                guard(t + 1 <= far, lambda: self.hop(way, t + 1, sub).start())
                self.across(way, t, sub).start()

            guard(t <= far, take)

    def all_parts(self):
        for t in range(1, self.far + 1):
            for sub in range(2):
                for way in ((sub,) if t == self.far else (0, 1)):
                    yield way, t, sub

    def finish(self):
        for sub in range(2):
            self.across(0, 0, sub).wait()
        for way, t, sub in self.all_parts():
            self.hop(way, t, sub).wait_send()
            self.across(way, t, sub).wait()


def ring_scratch(mesh_shape, rows, depth):
    far = mesh_shape['dp'] // 2 * mesh_shape['tp'] // 2
    return [pltpu.VMEM((rows, depth), jnp.bfloat16), pltpu.SemaphoreType.DMA((2,))] + [
        pltpu.SemaphoreType.DMA((2, far + 1, 2))] * 4


def norm_call(x, gain, shard, mesh_shape):
    n_tok, d = x.shape
    rows = shard.shape[0]
    n_dev = mesh_shape['dp'] * mesh_shape['tp']
    tt = 256
    n_t = n_tok // tt

    def body(x_ref, gain_ref, shard_ref, h_ref, ht_ref, out_ref, xbuf, hbuf, tbuf, xsem, hsem, tsem, *ring_refs):
        ring = Ring(mesh_shape, shard_ref, out_ref, *ring_refs)

        def load(i):
            return pltpu.make_async_copy(x_ref.at[pl.ds(i * tt, tt), :], xbuf.at[i % 2], xsem.at[i % 2])

        def put(i):
            return [pltpu.make_async_copy(hbuf.at[i % 2], h_ref.at[pl.ds(i * tt, tt), :], hsem.at[i % 2]),
                    pltpu.make_async_copy(tbuf.at[i % 2], ht_ref.at[:, pl.ds(i * tt, tt)], tsem.at[i % 2])]

        load(0).start()
        ring.begin()
        own = None
        events = [(t, sub) for t in range(1, ring.far + 1) for sub in range(2)]
        per = len(events) // n_t
        for i in range(n_t):
            if i + 1 < n_t:
                load(i + 1).start()
            load(i).wait()
            if i >= 2:
                for c in put(i - 2):
                    c.wait()
            wide = xbuf[i % 2].astype(jnp.float32)
            centered = wide - jnp.mean(wide, axis=-1, keepdims=True)
            var = jnp.mean(centered * centered, axis=-1, keepdims=True)
            h = centered * lax.rsqrt(var + LN_EPS) * gain_ref[...]
            hbuf[i % 2] = h.astype(jnp.bfloat16)
            tbuf[i % 2] = h.T.astype(jnp.bfloat16)
            for c in put(i):
                c.start()
            if i == 0:
                own = ring.keep_own()
                own.start()
            for ev in events[i * per:(i + 1) * per]:
                ring.event(*ev)
        for ev in events[n_t * per:]:
            ring.event(*ev)
        for i in (n_t - 2, n_t - 1):
            for c in put(i):
                c.wait()
        own.wait()
        ring.finish()

    any_spec = pl.BlockSpec(memory_space=pl.ANY)
    return pl.pallas_call(
        body,
        in_specs=[any_spec, pl.BlockSpec(memory_space=pltpu.VMEM), any_spec],
        out_specs=[any_spec] * 3,
        out_shape=[jax.ShapeDtypeStruct((n_tok, d), jnp.bfloat16), jax.ShapeDtypeStruct((d, n_tok), jnp.bfloat16),
                   jax.ShapeDtypeStruct((n_dev * rows, d), jnp.bfloat16)],
        scratch_shapes=[pltpu.VMEM((2, tt, d), jnp.bfloat16), pltpu.VMEM((2, tt, d), jnp.bfloat16),
                        pltpu.VMEM((2, d, tt), jnp.bfloat16)] + [pltpu.SemaphoreType.DMA((2,))] * 3
        + ring_scratch(mesh_shape, rows, d),
        compiler_params=pltpu.CompilerParams(collective_id=0, has_side_effects=True, vmem_limit_bytes=40 * 1024 * 1024),
        cost_estimate=pl.CostEstimate(flops=30 * 10 ** 9, bytes_accessed=n_tok * d * 6, transcendentals=0),
        name="norm",
    )(x, gain[None, :], shard)


def attention_call(rows, k_arr, v_arr, cos_tab, sin_tab, n_heads, head_dim, fresh_k):
    seq_len = rows.shape[0]
    half = head_dim // 2
    tq, kstep, pair = 256, 512, 2
    n_q, n_len = seq_len // tq, seq_len // kstep
    scale = (head_dim ** -0.5) * 1.4426950408889634

    def rope(a, cos, sin):
        a = a.astype(jnp.float32)
        lo, hi = a[:, :half], a[:, half:]
        return jnp.concatenate([lo * cos - hi * sin, hi * cos + lo * sin], axis=1).astype(jnp.bfloat16)

    def body(q_ref, k_ref, v_ref, cos_ref, sin_ref, o_ref, *caches):
        qi, hp = pl.program_id(0), pl.program_id(1)
        ks_ref, vs_ref = caches if fresh_k else (k_ref, v_ref)

        if fresh_k:
            @pl.when(jnp.logical_and(qi == 0, hp == 0))
            def _():
                def one(j, c):
                    r = pl.ds(pl.multiple_of(j * kstep, kstep), kstep)
                    ks_ref[r, :] = rope(k_ref[r, :], cos_ref[r, :], sin_ref[r, :])
                    vs_ref[r, :] = v_ref[r, :]
                    return c

                lax.fori_loop(0, n_len, one, 0)

        trow = pl.ds(pl.multiple_of(qi * tq, tq), tq)
        cos, sin = cos_ref[trow, :], sin_ref[trow, :]

        def span(length):
            keys = ks_ref[0:length, :]
            vals = vs_ref[0:length, :]
            k_pos = (length - kstep) + lax.broadcasted_iota(jnp.int32, (tq, kstep), 1)
            q_pos = qi * tq + lax.broadcasted_iota(jnp.int32, (tq, kstep), 0)
            allowed = k_pos <= q_pos
            for j in range(pair):
                cols = slice(j * head_dim, (j + 1) * head_dim)
                q = rope(q_ref[:, cols], cos, sin)
                s = lax.dot_general(q, keys, (((1,), (1,)), ((), ())), preferred_element_type=jnp.float32) * scale
                last = jnp.where(allowed, s[:, length - kstep:], -1e30)
                s = jnp.concatenate([s[:, :length - kstep], last], axis=1) if length > kstep else last
                top = jnp.max(s, axis=1, keepdims=True)
                e = jnp.exp2(s - top)
                tot = jnp.sum(e, axis=1, keepdims=True)
                pr = (e * (1.0 / tot)).astype(jnp.bfloat16)
                o_ref[:, cols] = jnp.dot(pr, vals, preferred_element_type=jnp.float32).astype(jnp.bfloat16)

        for b in range(n_len):
            pl.when(qi // (kstep // tq) == b)(functools.partial(span, (b + 1) * kstep))

    whole = pl.BlockSpec((seq_len, head_dim), lambda i, h: (0, 0))
    tab = pl.BlockSpec((seq_len, half), lambda i, h: (0, 0))
    out_specs = [pl.BlockSpec((tq, pair * head_dim), lambda i, h: (i, h))]
    out_shape = [jax.ShapeDtypeStruct((seq_len, n_heads * head_dim), jnp.bfloat16)]
    if fresh_k:
        k_arr = v_arr = rows
        kv_specs = [pl.BlockSpec((seq_len, head_dim), lambda i, h: (0, n_heads)),
                    pl.BlockSpec((seq_len, head_dim), lambda i, h: (0, n_heads + 1))]
        out_specs += [whole, whole]
        out_shape += [jax.ShapeDtypeStruct((seq_len, head_dim), jnp.bfloat16)] * 2
    else:
        kv_specs = [whole, whole]
    flops = 4 * n_heads * seq_len * seq_len * head_dim * 5 // 8
    return pl.pallas_call(
        body,
        grid=(n_q, n_heads // pair),
        in_specs=[pl.BlockSpec((tq, pair * head_dim), lambda i, h: (i, h))] + kv_specs + [tab, tab],
        out_specs=out_specs,
        out_shape=out_shape,
        compiler_params=pltpu.CompilerParams(dimension_semantics=("arbitrary", "arbitrary"),
                                             vmem_limit_bytes=40 * 1024 * 1024),
        cost_estimate=pl.CostEstimate(flops=flops, bytes_accessed=16 * 1024 * 1024, transcendentals=0),
        name="mqa_a" if fresh_k else "mqa_b",
    )(rows, k_arr, v_arr, cos_tab, sin_tab)


def in_proj_call(chunk, h_t, p_t, shard, first, mesh_shape, block, offset, collective_id):
    n_dev = mesh_shape['dp'] * mesh_shape['tp']
    rows = chunk.shape[0] // n_dev
    depth, n_tok = h_t.shape
    n_grp = n_dev - first
    g = next(c for c in (7, 4, 2, 1) if n_grp % c == 0 and c * rows <= 1280)
    steps = n_grp // g
    m = g * rows
    tn = min(1024, n_tok)
    n_n = n_tok // tn
    n_in = 2 + (p_t is not None) + (shard is not None)
    n_out = 1 + (shard is not None)

    def body(*refs):
        chunk_ref, h_ref = refs[0], refs[1]
        out_ref = refs[n_in]
        lbuf, obuf, lsem, osem = refs[n_in + n_out:n_in + n_out + 4]
        ring = None
        if shard is not None:
            ring = Ring(mesh_shape, refs[n_in - 1], refs[n_in + 1], *refs[n_in + n_out + 4:])

        def load(s):
            slot = s % 2 if isinstance(s, int) else lax.rem(s, 2)
            row = first * rows + s * m
            row = row if isinstance(s, int) else pl.multiple_of(row, UNIT)
            return pltpu.make_async_copy(chunk_ref.at[pl.ds(row, m), :], lbuf.at[slot], lsem.at[slot])

        def stores(s):
            slot = s % 2 if isinstance(s, int) else lax.rem(s, 2)
            to = [(s * g + i) * block + offset for i in range(g)]
            to = to if isinstance(s, int) else [pl.multiple_of(r, UNIT) for r in to]
            return [pltpu.make_async_copy(obuf.at[slot, pl.ds(i * rows, rows), :], out_ref.at[pl.ds(to[i], rows), :],
                                          osem.at[slot, i]) for i in range(g)]

        load(0).start()
        own = None
        if ring is not None:
            ring.begin()
            own = ring.keep_own()
            own.start()
            assert steps * n_n == ring.far

        def tick(it, carry):
            s, n = lax.div(it, n_n), lax.rem(it, n_n)
            slot = lax.rem(s, 2)

            @pl.when(n == 0)
            def _():
                @pl.when(s + 1 < steps)
                def _():
                    load(s + 1).start()

                load(s).wait()

                @pl.when(s >= 2)
                def _():
                    for c in stores(s - 2):
                        c.wait()

            cols = pl.ds(pl.multiple_of(n * tn, tn), tn)
            obuf[slot, :, cols] = jnp.dot(lbuf[slot], h_ref[:, cols],
                                          preferred_element_type=jnp.float32).astype(jnp.bfloat16)
            if ring is not None:
                for sub in range(2):
                    ring.event(it + 1, sub)

            @pl.when(n == n_n - 1)
            def _():
                for c in stores(s):
                    c.start()

            return carry

        lax.fori_loop(0, steps * n_n, tick, 0)
        for s in range(max(0, steps - 2), steps):
            for c in stores(s):
                c.wait()
        if ring is not None:
            own.wait()
            ring.finish()

    any_spec = pl.BlockSpec(memory_space=pl.ANY)
    args, specs, alias = [chunk, h_t], [any_spec, pl.BlockSpec(memory_space=pltpu.VMEM)], {}
    if p_t is not None:
        alias = {len(args): 0}
        args.append(p_t)
        specs.append(any_spec)
    out_shape = [jax.ShapeDtypeStruct((n_grp * block, n_tok), jnp.bfloat16)]
    scratch = [pltpu.VMEM((2, m, depth), jnp.bfloat16), pltpu.VMEM((2, m, n_tok), jnp.bfloat16),
               pltpu.SemaphoreType.DMA((2,)), pltpu.SemaphoreType.DMA((2, g))]
    kind = {}
    if shard is not None:
        args.append(shard)
        specs.append(any_spec)
        out_shape.append(jax.ShapeDtypeStruct((n_dev * shard.shape[0], depth), jnp.bfloat16))
        scratch += ring_scratch(mesh_shape, shard.shape[0], depth)
        kind = dict(collective_id=collective_id, has_side_effects=True)
    return pl.pallas_call(
        body,
        in_specs=specs,
        out_specs=[any_spec] * n_out,
        out_shape=out_shape,
        input_output_aliases=alias,
        scratch_shapes=scratch,
        compiler_params=pltpu.CompilerParams(vmem_limit_bytes=48 * 1024 * 1024, **kind),
        cost_estimate=pl.CostEstimate(flops=2 * n_grp * rows * depth * n_tok,
                                      bytes_accessed=2 * n_grp * rows * (depth + n_tok), transcendentals=0),
    )(*args)


PIECE = 64


def out_proj_call(p_t, w_chunk, at, per, per_dev, q_width, gate_at, ff, acc, last):
    n_tok, d_out = p_t.shape[1], w_chunk.shape[1]
    n_all = w_chunk.shape[0] // PIECE
    q_pieces = q_width // PIECE
    full, tail = 8, 4
    first = sum(1 for z in range(q_pieces) if at <= z % per_dev < at + per)
    count = n_all - first
    steps, rest = divmod(count, full)
    assert rest == tail and steps > 2
    kk = full * PIECE
    tt = min(512, n_tok)
    n_t = n_tok // tt

    def body(*refs):
        if last is None:
            p_ref, w_ref, out_ref, acc_ref, gbuf, ubuf, wbuf, sem, osem = refs
        else:
            (p_ref, w_ref, accin_ref, w0_ref, a0_ref, a1_ref, x_ref, out_ref,
             acc_ref, gbuf, ubuf, wbuf, sem, osem, abuf, xbuf, asem, xsem) = refs

        def copies(s, slot, n):
            row = pl.multiple_of((first + s * full) * PIECE, PIECE) if not isinstance(s, int) else (first + s * full) * PIECE
            res = [pltpu.make_async_copy(w_ref.at[pl.ds(row, n * PIECE), :],
                                         wbuf.at[slot, pl.ds(0, n * PIECE), :], sem.at[slot, 0])]
            for j in range(n):
                o = first + s * full + j
                dst = pl.ds(j * PIECE, PIECE)
                if isinstance(s, int):
                    row = gate_at + (per_dev * (o // per) + at + o % per - q_pieces) * PIECE
                else:
                    z = per_dev * lax.div(o, per) + at + lax.rem(o, per) - q_pieces
                    row = pl.multiple_of(gate_at + z * PIECE, PIECE)
                res.append(pltpu.make_async_copy(p_ref.at[pl.ds(row, PIECE), :], gbuf.at[slot, dst, :],
                                                 sem.at[slot, 1 + j]))
                res.append(pltpu.make_async_copy(p_ref.at[pl.ds(row + ff, PIECE), :], ubuf.at[slot, dst, :],
                                                 sem.at[slot, 1 + full + j]))
            return res

        def start(s, slot, n):
            for c in copies(s, slot, n):
                c.start()

        def finish(s, slot, n):
            for c in copies(s, slot, n):
                c.wait()

        def part(ref, t):
            return ref.at[pl.ds(t * tt, tt), :]

        def mlp(slot, n, fresh, before=None, after=None):
            k = n * PIECE
            for t in range(n_t):
                if before is not None:
                    before(t)
                tok = slice(t * tt, (t + 1) * tt)
                g = gbuf[slot, 0:k, tok].astype(jnp.float32)
                u = ubuf[slot, 0:k, tok].astype(jnp.float32)
                m = (g * (1.0 / (1.0 + jnp.exp(-g))) * u).astype(jnp.bfloat16)
                prod = lax.dot_general(m, wbuf[slot, 0:k, :], (((0,), (0,)), ((), ())), preferred_element_type=jnp.float32)
                if fresh:
                    acc_ref[tok, :] = prod
                else:
                    acc_ref[tok, :] += prod
                if after is not None:
                    after(t)

        start(0, 0, full)
        if last is not None:
            acc_in = [pltpu.make_async_copy(part(accin_ref, t), part(acc_ref, t), osem.at[t]) for t in range(n_t)]
            for c in acc_in:
                c.start()
            x_in = pltpu.make_async_copy(x_ref, xbuf, xsem.at[0])
            x_in.start()
        start(1, 1, full)
        finish(0, 0, full)
        mlp(0, full, last is None, (lambda t: acc_in[t].wait()) if last is not None else None)
        lo = 1

        def step(s, carry):
            slot = lax.rem(s, 2)

            @pl.when(s + 1 < steps)
            def _():
                start(s + 1, 1 - slot, full)

            @pl.when(s + 1 == steps)
            def _():
                start(steps, 1 - slot, tail)

            finish(s, slot, full)
            mlp(slot, full, False)
            return carry

        lax.fori_loop(lo, steps, step, 0)
        if last is not None:
            heads = a0_ref.shape[1] // kk
            srcs = [(a0_ref, i, 0) for i in range(heads)] + [(a1_ref, i, 1) for i in range(heads)]

            def attn_copies(i):
                ref, blk, odd = srcs[i]
                slot = (i + steps + 1) % 2
                res = [pltpu.make_async_copy(ref.at[:, pl.ds(blk * kk, kk)], abuf.at[slot], asem.at[slot, 0])]
                for j in range(full):
                    half, r = divmod(j, full // 2)
                    head = 2 * (2 * blk + half) + odd
                    z = head * (full // 2) + r
                    dev, loc = divmod(z, per_dev)
                    if loc < at:
                        src = w0_ref.at[pl.ds((dev * at + loc) * PIECE, PIECE), :]
                    else:
                        src = w_ref.at[pl.ds((dev * per + loc - at) * PIECE, PIECE), :]
                    res.append(pltpu.make_async_copy(src, wbuf.at[slot, pl.ds(j * PIECE, PIECE), :], asem.at[slot, 1 + j]))
                return res

            attn_copies_0 = attn_copies(0)
            for c in attn_copies_0:
                c.start()
        outs = []

        def put(src, t, sems):
            c = pltpu.make_async_copy(part(src, t), part(out_ref, t), sems.at[t])
            c.start()
            outs.append(c)

        finish(steps, steps % 2, tail)
        mlp(steps % 2, tail, False, None, (lambda t: put(acc_ref, t, osem)) if last is None else None)

        if last is not None:
            for i in range(len(srcs)):
                if i + 1 < len(srcs):
                    for c in attn_copies(i + 1):
                        c.start()
                for c in attn_copies(i):
                    c.wait()
                slot = (i + steps + 1) % 2
                if i + 1 == len(srcs):
                    x_in.wait()
                for t in range(n_t):
                    tok = slice(t * tt, (t + 1) * tt)
                    total = acc_ref[tok, :] + jnp.dot(abuf[slot, tok, :], wbuf[slot], preferred_element_type=jnp.float32)
                    if i + 1 < len(srcs):
                        acc_ref[tok, :] = total
                    else:
                        xbuf[tok, :] = (xbuf[tok, :].astype(jnp.float32) + total).astype(jnp.bfloat16)
                        put(xbuf, t, osem)
        for c in outs:
            c.wait()

    any_spec = pl.BlockSpec(memory_space=pl.ANY)
    args = [p_t, w_chunk]
    scratch = [pltpu.VMEM((n_tok, d_out), jnp.float32)] + [pltpu.VMEM((2, kk, n_tok), jnp.bfloat16)] * 2
    scratch += [pltpu.VMEM((2, kk, d_out), jnp.bfloat16), pltpu.SemaphoreType.DMA((2, 1 + 2 * full)),
                pltpu.SemaphoreType.DMA((n_t,))]
    out_dtype = jnp.float32
    if last is not None:
        w_first, a0, a1, x = last
        args += [acc, w_first, a0, a1, x]
        scratch += [pltpu.VMEM((2, n_tok, kk), jnp.bfloat16), pltpu.VMEM((n_tok, d_out), jnp.bfloat16),
                    pltpu.SemaphoreType.DMA((2, 1 + full)), pltpu.SemaphoreType.DMA((1,))]
        out_dtype = jnp.bfloat16
    k_total = count * PIECE + (q_width if last is not None else 0)
    return pl.pallas_call(
        body,
        in_specs=[any_spec] * len(args),
        out_specs=any_spec,
        out_shape=jax.ShapeDtypeStruct((n_tok, d_out), out_dtype),
        scratch_shapes=scratch,
        compiler_params=pltpu.CompilerParams(vmem_limit_bytes=60 * 1024 * 1024),
        cost_estimate=pl.CostEstimate(flops=2 * k_total * n_tok * d_out, bytes_accessed=6 * k_total * d_out, transcendentals=0),
        name="out_proj_b" if last is not None else "out_proj_a",
    )(*args)


EARLY_UNITS = (5, 8, 8)
FIRST_PIECES = 3


def solution(mesh):
    tok_spec = P(('part', 'dp', 'tp'))
    group = ('dp', 'tp')
    mesh_shape = dict(mesh.shape)
    n_dev = mesh_shape['dp'] * mesh_shape['tp']

    def gather(shard):
        return lax.all_gather(shard, group, axis=0, tiled=True)

    def per_device(x_blk, ln_gain, w_in_blk, w_out_blk):
        x = x_blk[0]
        seq_len, d_model = x.shape
        ff = 4 * d_model
        block = w_in_blk.shape[1]
        out_block = w_out_blk.shape[0]
        q_width = out_block * n_dev - ff
        head_dim = (block * n_dev - q_width - 2 * ff) // 2
        n_heads = q_width // head_dim
        n_qkv = q_width + 2 * head_dim
        first = n_qkv // block
        gate_at = n_qkv - first * block
        early_rows = block - head_dim
        cuts = [(2 * d + 1) * head_dim - d * block for d in range(first)]
        assert 2 * first == n_heads and all(0 <= c <= early_rows for c in cuts)
        assert sum(EARLY_UNITS) * UNIT == early_rows
        w_rows = w_in_blk.T
        me = lax.axis_index('dp') * mesh_shape['tp'] + lax.axis_index('tp')
        cut = jnp.where(me < first, head_dim - (block - 2 * head_dim) * me, early_rows)
        below = lax.broadcasted_iota(jnp.int32, (early_rows, 1), 0) < cut
        early_local = jnp.where(below, w_rows[:early_rows], w_rows[head_dim:])
        late_local = lax.dynamic_slice_in_dim(w_rows, cut, head_dim, axis=0)
        shards, at = [], 0
        for u in EARLY_UNITS:
            shards.append(early_local[at:at + u * UNIT])
            at += u * UNIT

        h, h_t, c0 = norm_call(x, ln_gain, shards[0], mesh_shape)
        cos_tab, sin_tab = rope_tables(seq_len, head_dim)

        def project(w):
            return lax.dot_general(h, w, (((1,), (1,)), ((), ())), preferred_element_type=jnp.float32).astype(jnp.bfloat16)

        offs = [sum(EARLY_UNITS[:i]) * UNIT for i in range(len(EARLY_UNITS) + 1)]
        p_t, c1 = in_proj_call(c0, h_t, None, shards[1], first, mesh_shape, block, offs[0], 1)
        late = gather(late_local)
        w_out_a = gather(w_out_blk[:FIRST_PIECES * PIECE])
        w_out_b = gather(w_out_blk[FIRST_PIECES * PIECE:])
        p_t, c2 = in_proj_call(c1, h_t, p_t, shards[2], first, mesh_shape, block, offs[1], 2)
        p_t = in_proj_call(c2, h_t, p_t, None, first, mesh_shape, block, offs[2], None)[0]
        early = (c0, c1, c2)
        tops = [c.reshape(n_dev, -1, d_model)[:first] for c in early]
        rest, left = [], gate_at
        for c in early:
            per = c.shape[0] // n_dev
            take = min(left, per)
            if take:
                rest.append(c[first * per:first * per + take])
            left -= take
        w_a = jnp.concatenate([jnp.concatenate(tops, axis=1).reshape(-1, d_model)] + rest, axis=0)
        attn_a, k_rot, v_all = attention_call(project(w_a), None, None, cos_tab, sin_tab, n_heads // 2, head_dim, True)
        p_t = in_proj_call(late, h_t, p_t, None, first, mesh_shape, block, offs[3], None)[0]
        attn_b = attention_call(project(late[:first * head_dim]), k_rot, v_all, cos_tab, sin_tab, n_heads // 2,
                                head_dim, False)[0]
        per_dev = out_block // PIECE
        acc = out_proj_call(p_t, w_out_a, 0, FIRST_PIECES, per_dev, q_width, gate_at, ff, None, None)
        y = out_proj_call(p_t, w_out_b, FIRST_PIECES, per_dev - FIRST_PIECES, per_dev, q_width, gate_at, ff, acc,
                          (w_out_a, attn_a, attn_b, x))
        return y[None], k_rot[None], v_all[None]

    return jax.shard_map(per_device, mesh=mesh,
                         in_specs=(tok_spec, P(), P(None, group), P(group, None)),
                         out_specs=(tok_spec, tok_spec, tok_spec), check_vma=False)
```

```python
import functools

import jax
import jax.numpy as jnp
from jax import lax
from jax.experimental import pallas as pl
from jax.experimental.pallas import tpu as pltpu
from jax.sharding import PartitionSpec as P


MESH = pl.DeviceIdType.MESH

LN_EPS = 1e-6
ROPE_BASE = 10000.0


def rope_tables(seq_len, head_dim):
    half = head_dim // 2
    inv_freq = ROPE_BASE ** (-jnp.arange(half, dtype=jnp.float32) * 2.0 / head_dim)
    angles = jnp.arange(seq_len, dtype=jnp.float32)[:, None] * inv_freq[None, :]
    return jnp.cos(angles), jnp.sin(angles)


UNIT = 16


class Ring:
    def __init__(self, mesh_shape, shard_ref, out_ref, stage, lsem, sends, recvs, sib_sends, sib_recvs):
        self.n = mesh_shape['tp']
        self.size = mesh_shape['dp'] // 2 * self.n
        assert mesh_shape['dp'] // 2 == self.n and self.size % 2 == 0
        self.far = self.size // 2
        self.shard, self.out, self.stage, self.lsem = shard_ref, out_ref, stage, lsem
        self.sends, self.recvs, self.sib_sends, self.sib_recvs = sends, recvs, sib_sends, sib_recvs
        self.rows = shard_ref.shape[0]
        top = (self.rows // UNIT + 1) // 2 * UNIT
        self.parts = ((0, top), (top, self.rows - top))
        self.dp, self.tp = lax.axis_index('dp'), lax.axis_index('tp')
        self.core = lax.rem(self.dp, 2)
        x = lax.div(self.dp, 2)
        a = x * (1 - self.core) + self.tp * self.core
        other = self.tp * (1 - self.core) + x * self.core
        self.pos = a * self.n + lax.rem(other + a, self.n)
        self.sibling = {'dp': self.dp + 1 - 2 * self.core, 'tp': self.tp}

    def at(self, pos):
        pos = lax.rem(pos + 2 * self.size, self.size)
        a = lax.div(pos, self.n)
        other = lax.rem(lax.rem(pos, self.n) + (self.n - 1) * a, self.n)
        x = a * (1 - self.core) + other * self.core
        y = other * (1 - self.core) + a * self.core
        return 2 * x + self.core, y

    def device(self, pos):
        dp, tp = self.at(pos)
        return {'dp': dp, 'tp': tp}

    def slot(self, pos, sub):
        dp, tp = self.at(pos)
        lo, n = self.parts[sub]
        return self.out.at[pl.ds(pl.multiple_of((dp * self.n + tp) * self.rows + lo, UNIT), n), :]

    def owner(self, way, t):
        return self.pos - t if way == 0 else self.pos + t

    def hop(self, way, t, sub):
        lo, n = self.parts[sub]
        dst = self.slot(self.owner(way, t - 1), sub)
        src = dst
        if isinstance(t, int) and t == 1:
            src = self.shard.at[pl.ds(lo, n), :]
        return pltpu.make_async_remote_copy(
            src_ref=src, dst_ref=dst, send_sem=self.sends.at[way, t, sub], recv_sem=self.recvs.at[way, t, sub],
            device_id=self.device(self.pos + 1 if way == 0 else self.pos - 1), device_id_type=MESH)

    def across(self, way, t, sub):
        lo, n = self.parts[sub]
        dst = self.slot(self.owner(way, t), sub)
        src = self.shard.at[pl.ds(lo, n), :] if isinstance(t, int) and t == 0 else dst
        return pltpu.make_async_remote_copy(
            src_ref=src, dst_ref=dst, send_sem=self.sib_sends.at[way, t, sub], recv_sem=self.sib_recvs.at[way, t, sub],
            device_id=self.sibling, device_id_type=MESH)

    def begin(self):
        barrier = pltpu.get_barrier_semaphore()
        for dev in (self.device(self.pos + 1), self.device(self.pos - 1), self.sibling):
            pl.semaphore_signal(barrier, inc=1, device_id=dev, device_id_type=MESH)
        pl.semaphore_wait(barrier, 3)
        for sub in range(2):
            for way in range(2):
                self.hop(way, 1, sub).start()
        for sub in range(2):
            self.across(0, 0, sub).start()
        pltpu.make_async_copy(self.shard, self.stage, self.lsem.at[0]).start()

    def keep_own(self):
        pltpu.make_async_copy(self.shard, self.stage, self.lsem.at[0]).wait()
        dp, tp = self.at(self.pos)
        mine = self.out.at[pl.ds(pl.multiple_of((dp * self.n + tp) * self.rows, UNIT), self.rows), :]
        return pltpu.make_async_copy(self.stage, mine, self.lsem.at[1])

    def event(self, t, sub):
        def guard(cond, fn):
            if isinstance(cond, bool):
                if cond:
                    fn()
            else:
                pl.when(cond)(fn)

        for way in (0, 1):
            far = self.far if way == sub else self.far - 1

            def take(way=way, far=far):
                self.hop(way, t, sub).wait_recv()
                guard(t + 1 <= far, lambda: self.hop(way, t + 1, sub).start())
                self.across(way, t, sub).start()

            guard(t <= far, take)

    def all_parts(self):
        for t in range(1, self.far + 1):
            for sub in range(2):
                for way in ((sub,) if t == self.far else (0, 1)):
                    yield way, t, sub

    def finish(self):
        for sub in range(2):
            self.across(0, 0, sub).wait()
        for way, t, sub in self.all_parts():
            self.hop(way, t, sub).wait_send()
            self.across(way, t, sub).wait()


def ring_scratch(mesh_shape, rows, depth):
    far = mesh_shape['dp'] // 2 * mesh_shape['tp'] // 2
    return [pltpu.VMEM((rows, depth), jnp.bfloat16), pltpu.SemaphoreType.DMA((2,))] + [
        pltpu.SemaphoreType.DMA((2, far + 1, 2))] * 4


def norm_call(x, gain, shard, mesh_shape):
    n_tok, d = x.shape
    rows = shard.shape[0]
    n_dev = mesh_shape['dp'] * mesh_shape['tp']
    tt = 128
    n_t = n_tok // tt

    def body(x_ref, gain_ref, shard_ref, h_ref, ht_ref, out_ref, xbuf, hbuf, tbuf, xsem, hsem, tsem, *ring_refs):
        ring = Ring(mesh_shape, shard_ref, out_ref, *ring_refs)

        def load(i):
            return pltpu.make_async_copy(x_ref.at[pl.ds(i * tt, tt), :], xbuf.at[i % 2], xsem.at[i % 2])

        def put(i):
            return [pltpu.make_async_copy(hbuf.at[i % 2], h_ref.at[pl.ds(i * tt, tt), :], hsem.at[i % 2]),
                    pltpu.make_async_copy(tbuf.at[i % 2], ht_ref.at[:, pl.ds(i * tt, tt)], tsem.at[i % 2])]

        load(0).start()
        ring.begin()
        own = None
        events = [(t, sub) for t in range(1, ring.far + 1) for sub in range(2)]
        per = len(events) // n_t
        for i in range(n_t):
            if i + 1 < n_t:
                load(i + 1).start()
            load(i).wait()
            if i >= 2:
                for c in put(i - 2):
                    c.wait()
            wide = xbuf[i % 2].astype(jnp.float32)
            centered = wide - jnp.mean(wide, axis=-1, keepdims=True)
            var = jnp.mean(centered * centered, axis=-1, keepdims=True)
            h = centered * lax.rsqrt(var + LN_EPS) * gain_ref[...]
            hbuf[i % 2] = h.astype(jnp.bfloat16)
            tbuf[i % 2] = h.T.astype(jnp.bfloat16)
            for c in put(i):
                c.start()
            if i == 0:
                own = ring.keep_own()
                own.start()
            for ev in events[i * per:(i + 1) * per]:
                ring.event(*ev)
        for ev in events[n_t * per:]:
            ring.event(*ev)
        for i in (n_t - 2, n_t - 1):
            for c in put(i):
                c.wait()
        own.wait()
        ring.finish()

    any_spec = pl.BlockSpec(memory_space=pl.ANY)
    return pl.pallas_call(
        body,
        in_specs=[any_spec, pl.BlockSpec(memory_space=pltpu.VMEM), any_spec],
        out_specs=[any_spec] * 3,
        out_shape=[jax.ShapeDtypeStruct((n_tok, d), jnp.bfloat16), jax.ShapeDtypeStruct((d, n_tok), jnp.bfloat16),
                   jax.ShapeDtypeStruct((n_dev * rows, d), jnp.bfloat16)],
        scratch_shapes=[pltpu.VMEM((2, tt, d), jnp.bfloat16), pltpu.VMEM((2, tt, d), jnp.bfloat16),
                        pltpu.VMEM((2, d, tt), jnp.bfloat16)] + [pltpu.SemaphoreType.DMA((2,))] * 3
        + ring_scratch(mesh_shape, rows, d),
        compiler_params=pltpu.CompilerParams(collective_id=0, has_side_effects=True, vmem_limit_bytes=40 * 1024 * 1024),
        cost_estimate=pl.CostEstimate(flops=30 * 10 ** 9, bytes_accessed=n_tok * d * 6, transcendentals=0),
        name="norm",
    )(x, gain[None, :], shard)


def attention_call(rows, k_arr, v_arr, cos_tab, sin_tab, n_heads, head_dim, fresh_k):
    seq_len = rows.shape[0]
    half = head_dim // 2
    tq, kstep, pair = 256, 512, 2
    n_q, n_len = seq_len // tq, seq_len // kstep
    scale = (head_dim ** -0.5) * 1.4426950408889634

    def rope(a, cos, sin):
        a = a.astype(jnp.float32)
        lo, hi = a[:, :half], a[:, half:]
        return jnp.concatenate([lo * cos - hi * sin, hi * cos + lo * sin], axis=1).astype(jnp.bfloat16)

    def body(q_ref, k_ref, v_ref, cos_ref, sin_ref, o_ref, *caches):
        qi, hp = pl.program_id(0), pl.program_id(1)
        ks_ref, vs_ref = caches if fresh_k else (k_ref, v_ref)

        if fresh_k:
            @pl.when(jnp.logical_and(qi == 0, hp == 0))
            def _():
                def one(j, c):
                    r = pl.ds(pl.multiple_of(j * kstep, kstep), kstep)
                    ks_ref[r, :] = rope(k_ref[r, :], cos_ref[r, :], sin_ref[r, :])
                    vs_ref[r, :] = v_ref[r, :]
                    return c

                lax.fori_loop(0, n_len, one, 0)

        trow = pl.ds(pl.multiple_of(qi * tq, tq), tq)
        cos, sin = cos_ref[trow, :], sin_ref[trow, :]

        def span(length):
            keys = ks_ref[0:length, :]
            vals = vs_ref[0:length, :]
            k_pos = (length - kstep) + lax.broadcasted_iota(jnp.int32, (tq, kstep), 1)
            q_pos = qi * tq + lax.broadcasted_iota(jnp.int32, (tq, kstep), 0)
            allowed = k_pos <= q_pos
            for j in range(pair):
                cols = slice(j * head_dim, (j + 1) * head_dim)
                q = rope(q_ref[:, cols], cos, sin)
                s = lax.dot_general(q, keys, (((1,), (1,)), ((), ())), preferred_element_type=jnp.float32) * scale
                last = jnp.where(allowed, s[:, length - kstep:], -1e30)
                s = jnp.concatenate([s[:, :length - kstep], last], axis=1) if length > kstep else last
                top = jnp.max(s, axis=1, keepdims=True)
                e = jnp.exp2(s - top)
                tot = jnp.sum(e, axis=1, keepdims=True)
                pr = (e * (1.0 / tot)).astype(jnp.bfloat16)
                o_ref[:, cols] = jnp.dot(pr, vals, preferred_element_type=jnp.float32).astype(jnp.bfloat16)

        for b in range(n_len):
            pl.when(qi // (kstep // tq) == b)(functools.partial(span, (b + 1) * kstep))

    whole = pl.BlockSpec((seq_len, head_dim), lambda i, h: (0, 0))
    tab = pl.BlockSpec((seq_len, half), lambda i, h: (0, 0))
    out_specs = [pl.BlockSpec((tq, pair * head_dim), lambda i, h: (i, h))]
    out_shape = [jax.ShapeDtypeStruct((seq_len, n_heads * head_dim), jnp.bfloat16)]
    if fresh_k:
        k_arr = v_arr = rows
        kv_specs = [pl.BlockSpec((seq_len, head_dim), lambda i, h: (0, n_heads)),
                    pl.BlockSpec((seq_len, head_dim), lambda i, h: (0, n_heads + 1))]
        out_specs += [whole, whole]
        out_shape += [jax.ShapeDtypeStruct((seq_len, head_dim), jnp.bfloat16)] * 2
    else:
        kv_specs = [whole, whole]
    flops = 4 * n_heads * seq_len * seq_len * head_dim * 5 // 8
    return pl.pallas_call(
        body,
        grid=(n_q, n_heads // pair),
        in_specs=[pl.BlockSpec((tq, pair * head_dim), lambda i, h: (i, h))] + kv_specs + [tab, tab],
        out_specs=out_specs,
        out_shape=out_shape,
        compiler_params=pltpu.CompilerParams(dimension_semantics=("arbitrary", "arbitrary"),
                                             vmem_limit_bytes=40 * 1024 * 1024),
        cost_estimate=pl.CostEstimate(flops=flops, bytes_accessed=16 * 1024 * 1024, transcendentals=0),
        name="mqa_a" if fresh_k else "mqa_b",
    )(rows, k_arr, v_arr, cos_tab, sin_tab)


def in_proj_call(chunk, h_t, p_t, shard, first, mesh_shape, block, offset, collective_id):
    n_dev = mesh_shape['dp'] * mesh_shape['tp']
    rows = chunk.shape[0] // n_dev
    depth, n_tok = h_t.shape
    n_grp = n_dev - first
    g = next(c for c in (7, 4, 2, 1) if n_grp % c == 0 and c * rows <= 1280)
    steps = n_grp // g
    m = g * rows
    tn = min(512, n_tok) if shard is not None else min(1024, n_tok)
    n_n = n_tok // tn
    n_in = 2 + (p_t is not None) + (shard is not None)
    n_out = 1 + (shard is not None)

    def body(*refs):
        chunk_ref, h_ref = refs[0], refs[1]
        out_ref = refs[n_in]
        lbuf, obuf, lsem, osem = refs[n_in + n_out:n_in + n_out + 4]
        ring = None
        if shard is not None:
            ring = Ring(mesh_shape, refs[n_in - 1], refs[n_in + 1], *refs[n_in + n_out + 4:])

        def load(s):
            slot = s % 2 if isinstance(s, int) else lax.rem(s, 2)
            row = first * rows + s * m
            row = row if isinstance(s, int) else pl.multiple_of(row, UNIT)
            return pltpu.make_async_copy(chunk_ref.at[pl.ds(row, m), :], lbuf.at[slot], lsem.at[slot])

        def stores(s):
            slot = s % 2 if isinstance(s, int) else lax.rem(s, 2)
            to = [(s * g + i) * block + offset for i in range(g)]
            to = to if isinstance(s, int) else [pl.multiple_of(r, UNIT) for r in to]
            return [pltpu.make_async_copy(obuf.at[slot, pl.ds(i * rows, rows), :], out_ref.at[pl.ds(to[i], rows), :],
                                          osem.at[slot, i]) for i in range(g)]

        load(0).start()
        own = None
        if ring is not None:
            ring.begin()
            own = ring.keep_own()
            own.start()
            assert steps * n_n == 2 * ring.far

        def tick(it, carry):
            s, n = lax.div(it, n_n), lax.rem(it, n_n)
            slot = lax.rem(s, 2)

            @pl.when(n == 0)
            def _():
                @pl.when(s + 1 < steps)
                def _():
                    load(s + 1).start()

                load(s).wait()

                @pl.when(s >= 2)
                def _():
                    for c in stores(s - 2):
                        c.wait()

            cols = pl.ds(pl.multiple_of(n * tn, tn), tn)
            obuf[slot, :, cols] = jnp.dot(lbuf[slot], h_ref[:, cols],
                                          preferred_element_type=jnp.float32).astype(jnp.bfloat16)
            if ring is not None:
                for sub in range(2):
                    @pl.when(lax.rem(it, 2) == sub)
                    def _(sub=sub):
                        ring.event(lax.div(it, 2) + 1, sub)

            @pl.when(n == n_n - 1)
            def _():
                for c in stores(s):
                    c.start()

            return carry

        lax.fori_loop(0, steps * n_n, tick, 0)
        for s in range(max(0, steps - 2), steps):
            for c in stores(s):
                c.wait()
        if ring is not None:
            own.wait()
            ring.finish()

    any_spec = pl.BlockSpec(memory_space=pl.ANY)
    args, specs, alias = [chunk, h_t], [any_spec, pl.BlockSpec(memory_space=pltpu.VMEM)], {}
    if p_t is not None:
        alias = {len(args): 0}
        args.append(p_t)
        specs.append(any_spec)
    out_shape = [jax.ShapeDtypeStruct((n_grp * block, n_tok), jnp.bfloat16)]
    scratch = [pltpu.VMEM((2, m, depth), jnp.bfloat16), pltpu.VMEM((2, m, n_tok), jnp.bfloat16),
               pltpu.SemaphoreType.DMA((2,)), pltpu.SemaphoreType.DMA((2, g))]
    kind = {}
    if shard is not None:
        args.append(shard)
        specs.append(any_spec)
        out_shape.append(jax.ShapeDtypeStruct((n_dev * shard.shape[0], depth), jnp.bfloat16))
        scratch += ring_scratch(mesh_shape, shard.shape[0], depth)
        kind = dict(collective_id=collective_id, has_side_effects=True)
    return pl.pallas_call(
        body,
        in_specs=specs,
        out_specs=[any_spec] * n_out,
        out_shape=out_shape,
        input_output_aliases=alias,
        scratch_shapes=scratch,
        compiler_params=pltpu.CompilerParams(vmem_limit_bytes=48 * 1024 * 1024, **kind),
        cost_estimate=pl.CostEstimate(flops=2 * n_grp * rows * depth * n_tok,
                                      bytes_accessed=2 * n_grp * rows * (depth + n_tok), transcendentals=0),
    )(*args)


PIECE = 64


def out_proj_call(p_t, w_chunk, at, per, per_dev, q_width, gate_at, ff, acc, last):
    n_tok, d_out = p_t.shape[1], w_chunk.shape[1]
    n_all = w_chunk.shape[0] // PIECE
    q_pieces = q_width // PIECE
    full, tail = 8, 4
    first = sum(1 for z in range(q_pieces) if at <= z % per_dev < at + per)
    count = n_all - first
    steps, rest = divmod(count, full)
    assert rest == tail and steps > 2
    kk = full * PIECE
    tt = min(512, n_tok)
    n_t = n_tok // tt

    def body(*refs):
        if last is None:
            p_ref, w_ref, out_ref, acc_ref, gbuf, ubuf, wbuf, sem, osem = refs
        else:
            (p_ref, w_ref, accin_ref, w0_ref, a0_ref, a1_ref, x_ref, out_ref,
             acc_ref, gbuf, ubuf, wbuf, sem, osem, abuf, xbuf, asem, xsem) = refs

        def copies(s, slot, n):
            row = pl.multiple_of((first + s * full) * PIECE, PIECE) if not isinstance(s, int) else (first + s * full) * PIECE
            res = [pltpu.make_async_copy(w_ref.at[pl.ds(row, n * PIECE), :],
                                         wbuf.at[slot, pl.ds(0, n * PIECE), :], sem.at[slot, 0])]
            for j in range(n):
                o = first + s * full + j
                dst = pl.ds(j * PIECE, PIECE)
                if isinstance(s, int):
                    row = gate_at + (per_dev * (o // per) + at + o % per - q_pieces) * PIECE
                else:
                    z = per_dev * lax.div(o, per) + at + lax.rem(o, per) - q_pieces
                    row = pl.multiple_of(gate_at + z * PIECE, PIECE)
                res.append(pltpu.make_async_copy(p_ref.at[pl.ds(row, PIECE), :], gbuf.at[slot, dst, :],
                                                 sem.at[slot, 1 + j]))
                res.append(pltpu.make_async_copy(p_ref.at[pl.ds(row + ff, PIECE), :], ubuf.at[slot, dst, :],
                                                 sem.at[slot, 1 + full + j]))
            return res

        def start(s, slot, n):
            for c in copies(s, slot, n):
                c.start()

        def finish(s, slot, n):
            for c in copies(s, slot, n):
                c.wait()

        def part(ref, t):
            return ref.at[pl.ds(t * tt, tt), :]

        def mlp(slot, n, fresh, before=None, after=None):
            k = n * PIECE
            for t in range(n_t):
                if before is not None:
                    before(t)
                tok = slice(t * tt, (t + 1) * tt)
                g = gbuf[slot, 0:k, tok].astype(jnp.float32)
                u = ubuf[slot, 0:k, tok].astype(jnp.float32)
                m = (g * (1.0 / (1.0 + jnp.exp(-g))) * u).astype(jnp.bfloat16)
                prod = lax.dot_general(m, wbuf[slot, 0:k, :], (((0,), (0,)), ((), ())), preferred_element_type=jnp.float32)
                if fresh:
                    acc_ref[tok, :] = prod
                else:
                    acc_ref[tok, :] += prod
                if after is not None:
                    after(t)

        start(0, 0, full)
        if last is not None:
            acc_in = [pltpu.make_async_copy(part(accin_ref, t), part(acc_ref, t), osem.at[t]) for t in range(n_t)]
            for c in acc_in:
                c.start()
            x_in = pltpu.make_async_copy(x_ref, xbuf, xsem.at[0])
            x_in.start()
        start(1, 1, full)
        finish(0, 0, full)
        mlp(0, full, last is None, (lambda t: acc_in[t].wait()) if last is not None else None)
        lo = 1

        def step(s, carry):
            slot = lax.rem(s, 2)

            @pl.when(s + 1 < steps)
            def _():
                start(s + 1, 1 - slot, full)

            @pl.when(s + 1 == steps)
            def _():
                start(steps, 1 - slot, tail)

            finish(s, slot, full)
            mlp(slot, full, False)
            return carry

        lax.fori_loop(lo, steps, step, 0)
        if last is not None:
            heads = a0_ref.shape[1] // kk
            srcs = [(a0_ref, i, 0) for i in range(heads)] + [(a1_ref, i, 1) for i in range(heads)]

            def attn_copies(i):
                ref, blk, odd = srcs[i]
                slot = (i + steps + 1) % 2
                res = [pltpu.make_async_copy(ref.at[:, pl.ds(blk * kk, kk)], abuf.at[slot], asem.at[slot, 0])]
                for j in range(full):
                    half, r = divmod(j, full // 2)
                    head = 2 * (2 * blk + half) + odd
                    z = head * (full // 2) + r
                    dev, loc = divmod(z, per_dev)
                    if loc < at:
                        src = w0_ref.at[pl.ds((dev * at + loc) * PIECE, PIECE), :]
                    else:
                        src = w_ref.at[pl.ds((dev * per + loc - at) * PIECE, PIECE), :]
                    res.append(pltpu.make_async_copy(src, wbuf.at[slot, pl.ds(j * PIECE, PIECE), :], asem.at[slot, 1 + j]))
                return res

            attn_copies_0 = attn_copies(0)
            for c in attn_copies_0:
                c.start()
        outs = []

        def put(src, t, sems):
            c = pltpu.make_async_copy(part(src, t), part(out_ref, t), sems.at[t])
            c.start()
            outs.append(c)

        finish(steps, steps % 2, tail)
        mlp(steps % 2, tail, False, None, (lambda t: put(acc_ref, t, osem)) if last is None else None)

        if last is not None:
            for i in range(len(srcs)):
                if i + 1 < len(srcs):
                    for c in attn_copies(i + 1):
                        c.start()
                for c in attn_copies(i):
                    c.wait()
                slot = (i + steps + 1) % 2
                if i + 1 == len(srcs):
                    x_in.wait()
                for t in range(n_t):
                    tok = slice(t * tt, (t + 1) * tt)
                    total = acc_ref[tok, :] + jnp.dot(abuf[slot, tok, :], wbuf[slot], preferred_element_type=jnp.float32)
                    if i + 1 < len(srcs):
                        acc_ref[tok, :] = total
                    else:
                        xbuf[tok, :] = (xbuf[tok, :].astype(jnp.float32) + total).astype(jnp.bfloat16)
                        put(xbuf, t, osem)
        for c in outs:
            c.wait()

    any_spec = pl.BlockSpec(memory_space=pl.ANY)
    args = [p_t, w_chunk]
    scratch = [pltpu.VMEM((n_tok, d_out), jnp.float32)] + [pltpu.VMEM((2, kk, n_tok), jnp.bfloat16)] * 2
    scratch += [pltpu.VMEM((2, kk, d_out), jnp.bfloat16), pltpu.SemaphoreType.DMA((2, 1 + 2 * full)),
                pltpu.SemaphoreType.DMA((n_t,))]
    out_dtype = jnp.float32
    if last is not None:
        w_first, a0, a1, x = last
        args += [acc, w_first, a0, a1, x]
        scratch += [pltpu.VMEM((2, n_tok, kk), jnp.bfloat16), pltpu.VMEM((n_tok, d_out), jnp.bfloat16),
                    pltpu.SemaphoreType.DMA((2, 1 + full)), pltpu.SemaphoreType.DMA((1,))]
        out_dtype = jnp.bfloat16
    k_total = count * PIECE + (q_width if last is not None else 0)
    return pl.pallas_call(
        body,
        in_specs=[any_spec] * len(args),
        out_specs=any_spec,
        out_shape=jax.ShapeDtypeStruct((n_tok, d_out), out_dtype),
        scratch_shapes=scratch,
        compiler_params=pltpu.CompilerParams(vmem_limit_bytes=60 * 1024 * 1024),
        cost_estimate=pl.CostEstimate(flops=2 * k_total * n_tok * d_out, bytes_accessed=6 * k_total * d_out, transcendentals=0),
        name="out_proj_b" if last is not None else "out_proj_a",
    )(*args)


EARLY_UNITS = (5, 8, 8)
FIRST_PIECES = 3


def solution(mesh):
    tok_spec = P(('part', 'dp', 'tp'))
    group = ('dp', 'tp')
    mesh_shape = dict(mesh.shape)
    n_dev = mesh_shape['dp'] * mesh_shape['tp']

    def gather(shard):
        return lax.all_gather(shard, group, axis=0, tiled=True)

    def per_device(x_blk, ln_gain, w_in_blk, w_out_blk):
        x = x_blk[0]
        seq_len, d_model = x.shape
        ff = 4 * d_model
        block = w_in_blk.shape[1]
        out_block = w_out_blk.shape[0]
        q_width = out_block * n_dev - ff
        head_dim = (block * n_dev - q_width - 2 * ff) // 2
        n_heads = q_width // head_dim
        n_qkv = q_width + 2 * head_dim
        first = n_qkv // block
        gate_at = n_qkv - first * block
        early_rows = block - head_dim
        cuts = [(2 * d + 1) * head_dim - d * block for d in range(first)]
        assert 2 * first == n_heads and all(0 <= c <= early_rows for c in cuts)
        assert sum(EARLY_UNITS) * UNIT == early_rows
        w_rows = w_in_blk.T
        me = lax.axis_index('dp') * mesh_shape['tp'] + lax.axis_index('tp')
        cut = jnp.where(me < first, head_dim - (block - 2 * head_dim) * me, early_rows)
        below = lax.broadcasted_iota(jnp.int32, (early_rows, 1), 0) < cut
        early_local = jnp.where(below, w_rows[:early_rows], w_rows[head_dim:])
        late_local = lax.dynamic_slice_in_dim(w_rows, cut, head_dim, axis=0)
        shards, at = [], 0
        for u in EARLY_UNITS:
            shards.append(early_local[at:at + u * UNIT])
            at += u * UNIT

        h, h_t, c0 = norm_call(x, ln_gain, shards[0], mesh_shape)
        cos_tab, sin_tab = rope_tables(seq_len, head_dim)

        def project(w):
            return lax.dot_general(h, w, (((1,), (1,)), ((), ())), preferred_element_type=jnp.float32).astype(jnp.bfloat16)

        offs = [sum(EARLY_UNITS[:i]) * UNIT for i in range(len(EARLY_UNITS) + 1)]
        p_t, c1 = in_proj_call(c0, h_t, None, shards[1], first, mesh_shape, block, offs[0], 1)
        late = gather(late_local)
        w_out_a = gather(w_out_blk[:FIRST_PIECES * PIECE])
        w_out_b = gather(w_out_blk[FIRST_PIECES * PIECE:])
        p_t, c2 = in_proj_call(c1, h_t, p_t, shards[2], first, mesh_shape, block, offs[1], 2)
        p_t = in_proj_call(c2, h_t, p_t, None, first, mesh_shape, block, offs[2], None)[0]
        early = (c0, c1, c2)
        tops = [c.reshape(n_dev, -1, d_model)[:first] for c in early]
        rest, left = [], gate_at
        for c in early:
            per = c.shape[0] // n_dev
            take = min(left, per)
            if take:
                rest.append(c[first * per:first * per + take])
            left -= take
        w_a = jnp.concatenate([jnp.concatenate(tops, axis=1).reshape(-1, d_model)] + rest, axis=0)
        attn_a, k_rot, v_all = attention_call(project(w_a), None, None, cos_tab, sin_tab, n_heads // 2, head_dim, True)
        p_t = in_proj_call(late, h_t, p_t, None, first, mesh_shape, block, offs[3], None)[0]
        attn_b = attention_call(project(late[:first * head_dim]), k_rot, v_all, cos_tab, sin_tab, n_heads // 2,
                                head_dim, False)[0]
        per_dev = out_block // PIECE
        acc = out_proj_call(p_t, w_out_a, 0, FIRST_PIECES, per_dev, q_width, gate_at, ff, None, None)
        y = out_proj_call(p_t, w_out_b, FIRST_PIECES, per_dev - FIRST_PIECES, per_dev, q_width, gate_at, ff, acc,
                          (w_out_a, attn_a, attn_b, x))
        return y[None], k_rot[None], v_all[None]

    return jax.shard_map(per_device, mesh=mesh,
                         in_specs=(tok_spec, P(), P(None, group), P(group, None)),
                         out_specs=(tok_spec, tok_spec, tok_spec), check_vma=False)
```
